32 devices in a mesh: rows: 8 (over z, y), cols: 4 (over x, core).
Axes of the slice: x: 2, y: 2, z: 4, core: 2. Of those that a mesh axis runs over, the one named last changes fastest.
Arguments:
- latent: bfloat16 [4, 8, 1024], P(None, 'rows', 'cols'), may hold values from -18 to 18
- deep: bfloat16 [320, 8, 1024], P(None, 'rows', 'cols'), may hold values from -6 to 6
- timestep: int32 [1], replicated, may hold values from 0 to 999
- in_weight: bfloat16 [36, 320], replicated, may hold values from -1 to 1
- front_weight: bfloat16 [5760, 320], P('rows'), may hold values from -0.078125 to 0.078125
- middle_weight: bfloat16 [2880, 320], P('cols'), may hold values from -0.109375 to 0.109375
- skip_weight: bfloat16 [640, 320], P('cols'), may hold values from -0.25 to 0.25
- out_weight: bfloat16 [2880, 4], replicated, may hold values from -0.109375 to 0.109375
- time_weight: bfloat16 [320, 1280], replicated, may hold values from -0.3125 to 0.3125
- time_second: bfloat16 [1280, 1280], P('cols'), may hold values from -0.15625 to 0.15625
- time_proj: bfloat16 [1280, 320], replicated, may hold values from -0.15625 to 0.15625
- input_gain: float32 [640], replicated, may hold values from 0.1 to 1.9
- middle_gain: float32 [320], replicated, may hold values from 0.1 to 1.9
- output_gain: float32 [320], replicated, may hold values from 0.1 to 1.9
Outputs:
- noise: float32 [4, 8, 1024], P(None, 'rows', 'cols')
The draws below stay inside these ranges and needn't reach their ends.
All inputs are finite; a program needn't handle non-finite values.
Results may differ from the reference program's by a relative error of at most 0.0047.
Values may be sent and summed in bfloat16 or wider, within the bound.
A program may use at most 64 MiB of HBM per device.

```python
import math
import jax
import jax.numpy as jnp
from jax import lax

C = 320
CIN = 4
GROUPS = 32
FREQ = 320
TIME = 1280
H = 8
W = 1024


def draw_latent(key, part):
    key_base = jax.random.fold_in(key, 11)
    key_rough = jax.random.fold_in(key, 23)
    positions = jnp.arange(H, dtype=jnp.float32) / H
    rising = 3.0 ** positions
    rough = jax.random.uniform(key_rough, (CIN, H, W), jnp.float32, 0.5, 1.5)
    base = jnp.clip(jax.random.normal(key_base, (CIN, H, W), jnp.float32), -4.0, 4.0)
    return (base * rough * rising[None, :, None]).astype(jnp.bfloat16)


def draw_deep(key, part):
    map_count = 6
    wave_count = 3
    key_rowfreq = jax.random.fold_in(key, 101)
    key_colfreq = jax.random.fold_in(key, 103)
    key_phase = jax.random.fold_in(key, 107)
    key_amplitude = jax.random.fold_in(key, 109)
    key_loadings = jax.random.fold_in(key, 113)
    key_jitter = jax.random.fold_in(key, 127)
    key_offset = jax.random.fold_in(key, 131)
    freq_rows = jax.random.randint(key_rowfreq, (map_count, wave_count), 1, 5).astype(jnp.float32)
    freq_cols = jax.random.randint(key_colfreq, (map_count, wave_count), 1, 9).astype(jnp.float32)
    phases = jax.random.uniform(key_phase, (map_count, wave_count), jnp.float32, 0.0, 2.0 * math.pi)
    amplitude = jax.random.normal(key_amplitude, (map_count, wave_count), jnp.float32)
    row_pos = jnp.arange(H, dtype=jnp.float32) / H
    col_pos = jnp.arange(W, dtype=jnp.float32) / W
    smooth_maps = jnp.zeros((map_count, H, W), jnp.float32)
    for wave_index in range(wave_count):
        angle_grid = 2.0 * math.pi * (freq_rows[:, wave_index, None, None] * row_pos[None, :, None] + freq_cols[:, wave_index, None, None] * col_pos[None, None, :]) + phases[:, wave_index, None, None]
        smooth_maps = smooth_maps + amplitude[:, wave_index, None, None] * jnp.cos(angle_grid)
    map_norms = jnp.sqrt(0.5 * jnp.sum(amplitude * amplitude, axis=1) + 0.001)
    smooth_maps = smooth_maps / map_norms[:, None, None]
    loadings = jax.random.normal(key_loadings, (C, map_count), jnp.float32) * (1.1 / math.sqrt(map_count))
    common_part = jnp.einsum('ck,khw->chw', loadings, smooth_maps)
    offsets = 0.3 * jax.random.normal(key_offset, (C,), jnp.float32)
    jitter = 0.5 * jax.random.normal(key_jitter, (C, H, W), jnp.float32)
    result_value = common_part + jitter + offsets[:, None, None]
    return jnp.clip(result_value, -6.0, 6.0).astype(jnp.bfloat16)


def shard_levels(stream_key, shape, shards, smallest, largest):
    def one(dim, shards_of):
        steps = jax.random.uniform(jax.random.fold_in(jax.random.fold_in(stream_key, 6), dim), (shards_of,), jnp.float32, smallest / len(shards), largest / len(shards))
        return jnp.repeat(jnp.exp(steps), shape[dim] // shards_of).reshape((-1,) + (1,) * (len(shape) - dim - 1))

    level = one(*shards[0])
    for cut in shards[1:]:
        level = level * one(*cut)
    return level


def noise(key, shape, width, most, cuts=(), held_as=jnp.bfloat16):
    level = shard_levels(key, shape, cuts, -0.22, 0.18) if cuts else 1.0
    values = jax.random.normal(key, shape, jnp.float32) * width * level
    return jnp.minimum(jnp.maximum(values, -most), most).astype(held_as)


def setup_inputs(seed: int = 0) -> dict:
    seeds = jax.random.split(jax.random.key(seed), 15)
    latent = draw_latent(jax.random.fold_in(seeds[14], 71), 0)
    deep = draw_deep(jax.random.fold_in(seeds[14], 71), 0)
    timestep = jax.random.randint(seeds[2], (1,), 0, 1000).astype(jnp.int32)
    in_weight = noise(seeds[3], (9 * CIN, C), (9 * CIN) ** -0.5, 1.0)
    front_weight = noise(seeds[4], (18 * C, C), (18 * C) ** -0.5, 0.078125, ((0, 8),))
    middle_weight = noise(seeds[5], (9 * C, C), (9 * C) ** -0.5, 0.109375, ((0, 4),))
    skip_weight = noise(seeds[6], (2 * C, C), (2 * C) ** -0.5, 0.25, ((0, 4),))
    out_weight = noise(seeds[7], (9 * C, CIN), (9 * C) ** -0.5, 0.109375)
    time_weight = noise(seeds[8], (FREQ, TIME), FREQ ** -0.5, 0.3125)
    time_second = noise(seeds[9], (TIME, TIME), TIME ** -0.5, 0.15625, ((0, 4),))
    time_proj = noise(seeds[10], (TIME, C), TIME ** -0.5, 0.15625)
    input_gain = jnp.clip(1.0 + 0.18 * jax.random.normal(seeds[11], (2 * C,), jnp.float32), 0.1, 1.9)
    middle_gain = jnp.clip(1.0 + 0.18 * jax.random.normal(seeds[12], (C,), jnp.float32), 0.1, 1.9)
    output_gain = jnp.clip(1.0 + 0.18 * jax.random.normal(seeds[13], (C,), jnp.float32), 0.1, 1.9)
    return {"latent": latent, "deep": deep, "timestep": timestep, "in_weight": in_weight, "front_weight": front_weight, "middle_weight": middle_weight, "skip_weight": skip_weight, "out_weight": out_weight, "time_weight": time_weight, "time_second": time_second, "time_proj": time_proj, "input_gain": input_gain, "middle_gain": middle_gain, "output_gain": output_gain}


epsilon = 1e-05

def convolve(field, weight):
    channels = field.shape[0]
    kernel = weight.astype(jnp.float32).reshape(3, 3, channels, -1).transpose(3, 2, 0, 1)
    result = lax.conv_general_dilated(field.astype(jnp.float32)[None], kernel, (1, 1), ((1, 1), (1, 1)), dimension_numbers=('NCHW', 'OIHW', 'NCHW'), precision=lax.Precision.HIGHEST)
    return result[0]

def norm_silu(values, gain):
    grouped = values.reshape(GROUPS, -1)
    center = lax.optimization_barrier(jnp.mean(grouped, axis=1, keepdims=True))
    offsets = grouped - center
    spread = lax.optimization_barrier(jnp.mean(offsets * offsets, axis=1, keepdims=True))
    scaled = (offsets * lax.rsqrt(spread + epsilon)).reshape(values.shape) * gain[:, None, None]
    return jax.nn.silu(scaled).astype(jnp.bfloat16)

def time_shift_of(timestep, time_weight, time_second, time_proj):
    half_width = time_weight.shape[0] // 2
    ratios = jnp.exp(-math.log(10000.0) * jnp.arange(half_width, dtype=jnp.float32) / half_width)
    angles = timestep[0].astype(jnp.float32) * ratios
    features = jnp.concatenate([jnp.cos(angles), jnp.sin(angles)])
    hidden = jax.nn.silu(jnp.dot(features, time_weight.astype(jnp.float32), precision=lax.Precision.HIGHEST))
    embedded = jnp.dot(hidden, time_second.astype(jnp.float32), precision=lax.Precision.HIGHEST)
    return jnp.dot(jax.nn.silu(embedded), time_proj.astype(jnp.float32), precision=lax.Precision.HIGHEST)

def reference(latent, deep, timestep, in_weight, front_weight, middle_weight, skip_weight, out_weight, time_weight, time_second, time_proj, input_gain, middle_gain, output_gain):
    skip_feat = convolve(latent, in_weight).astype(jnp.bfloat16)
    joined = jnp.concatenate([deep, skip_feat], axis=0)
    act_one = norm_silu(joined.astype(jnp.float32), input_gain)
    time_shift = time_shift_of(timestep, time_weight, time_second, time_proj)
    hidden_one = convolve(act_one, front_weight) + time_shift[:, None, None]
    act_two = norm_silu(hidden_one, middle_gain)
    flat_joined = joined.reshape(joined.shape[0], -1)
    shortcut = jnp.dot(jnp.transpose(skip_weight), flat_joined, preferred_element_type=jnp.float32)
    shortcut = shortcut.reshape(-1, joined.shape[1], joined.shape[2])
    block_out = convolve(act_two, middle_weight) + shortcut
    act_three = norm_silu(block_out, output_gain)
    return convolve(act_three, out_weight)
```

```python
import functools
import math

import jax
import jax.numpy as jnp
from jax import lax
from jax.experimental import pallas as pl
from jax.experimental.pallas import tpu as pltpu
from jax.sharding import PartitionSpec as P

GROUPS = 32
EPS = 1e-05
TILE = 16
LANES = 128
MESH = pl.DeviceIdType.MESH
F32 = jnp.float32
BF16 = jnp.bfloat16
SIDES = tuple((i, j) for i in (-1, 0, 1) for j in (-1, 0, 1) if (i, j) != (0, 0))


def dot(a, b, precision=None):
    return lax.dot_general(
        a, b, (((1,), (0,)), ((), ())), preferred_element_type=F32, precision=precision
    )


def split_dot(row, weight):
    high = row.astype(BF16)
    rest = row - high.astype(F32)
    middle = rest.astype(BF16)
    low = (rest - middle.astype(F32)).astype(BF16)
    return dot(high, weight) + dot(middle, weight) + dot(low, weight)


def silu(z):
    return z / (1.0 + jnp.exp(-z))


def kernel(
    R, Q, ring,
    latent, deep, features, in_w, front, middle, skip, out_w, time_w, time_s, time_p,
    gain_one, gain_two, gain_three,
    noise,
    lat, jext, hext, oext, shifted, patch, fw, mw, sw, part, emb, sums_a, sums_b,
    lat_s, lat_r, halo_s, halo_r, fz_s, fy_s, fc_s, fm_r, fo_r, mid_s, mid_r, emb_s, emb_r,
    ca_s, ca_r, cb_s, cb_r, loc_s,
):
    r = lax.axis_index("rows")
    c = lax.axis_index("cols")
    C, px = deep.shape
    cin = latent.shape[0]
    image = float(px * R * Q)

    def remote(src, dst, ssem, rsem, rr, cc):
        return pltpu.make_async_remote_copy(
            src_ref=src, dst_ref=dst, send_sem=ssem, recv_sem=rsem,
            device_id={"rows": rr, "cols": cc}, device_id_type=MESH,
        )

    def each(count, body):
        if count <= 8:
            for i in range(1, count):
                body(i)
        else:
            lax.fori_loop(1, count, lambda i, u: (body(i), u)[1], 0)

    barrier = pltpu.get_barrier_semaphore()

    def greet(rr, cc):
        pl.semaphore_signal(barrier, inc=1, device_id={"rows": rr, "cols": cc}, device_id_type=MESH)

    each(R, lambda i: greet(lax.rem(r + i, R), c))
    each(Q, lambda i: greet(r, lax.rem(c + i, Q)))
    for i in (-1, 1):
        for j in (-1, 1):
            greet(lax.rem(r + i + R, R), lax.rem(c + j + Q, Q))
    pl.semaphore_wait(barrier, R - 1 + Q - 1 + 4)

    def inside(rr, cc):
        return (rr >= 0) & (rr < R) & (cc >= 0) & (cc < Q)

    def lat_copy(k, rr, cc):
        i, j = SIDES[k]
        return remote(latent, lat.at[k], lat_s.at[k], lat_r.at[k], rr, cc)

    for k, (i, j) in enumerate(SIDES):
        @pl.when(inside(r + i, c + j))
        def _():
            lat_copy(k, r + i, c + j).start()

        @pl.when(jnp.logical_not(inside(r - i, c - j)))
        def _():
            lat[k] = jnp.zeros(lat.shape[1:], lat.dtype)

    parity = lax.rem(c, 2)
    mate = c + 1 - 2 * parity
    over = lax.rem(c + 2, Q)
    half_c = lax.rem(r, 2)
    twin = r + 1 - 2 * half_c
    mk, sk = middle.shape[0], skip.shape[0]

    def mid_copies(owner, s, slot_from, target):
        rows_m = pl.ds(pl.multiple_of(owner * mk, TILE), mk)
        rows_s = pl.ds(pl.multiple_of(owner * sk, TILE), sk)
        src_m, src_s = (middle, skip) if slot_from else (mw.at[rows_m], sw.at[rows_s])
        return (
            remote(src_m, mw.at[rows_m], mid_s.at[0, s], mid_r.at[0, s], r, target),
            remote(src_s, sw.at[rows_s], mid_s.at[1, s], mid_r.at[1, s], r, target),
        )

    fk = fw.shape[0] // R if ring else 0
    cut = fk // 2 // TILE * TILE
    spans = ((0, cut), (cut, fk - cut))

    def f_rows(owner, par):
        return pl.ds(pl.multiple_of(owner * fk, TILE) + spans[par][0], spans[par][1])

    def by_parity(par_of, body):
        for par in (0, 1):
            @pl.when(par_of == par)
            def _():
                body(par)

    def f_own(par, target, ssem):
        src = front.at[pl.ds(spans[par][0], spans[par][1])]
        return remote(src, fw.at[f_rows(r, par)], ssem, fm_r.at[r], target, c)

    def f_pass(owner, par, target):
        return remote(fw.at[f_rows(owner, par)], fw.at[f_rows(owner, par)],
                      fy_s.at[owner], fm_r.at[owner], target, c)

    def f_mate(owner, par):
        return remote(fw.at[f_rows(owner, par)], fw.at[f_rows(owner, par)],
                      fc_s.at[owner], fo_r.at[owner], r, mate)

    locals_ = []
    if ring:
        locals_.append(pltpu.make_async_copy(
            front, fw.at[pl.ds(pl.multiple_of(r * fk, TILE), fk)], loc_s.at[0]))
    locals_.append(pltpu.make_async_copy(
        middle, mw.at[pl.ds(pl.multiple_of(c * mk, TILE), mk)], loc_s.at[1]))
    locals_.append(pltpu.make_async_copy(
        skip, sw.at[pl.ds(pl.multiple_of(c * sk, TILE), sk)], loc_s.at[2]))
    for copy in locals_:
        copy.start()

    if ring:
        def first(par):
            f_own(par, twin, fy_s.at[r]).start()
            for i in range(1, R // 2):
                t = lax.rem(r + 2 * i, R)
                f_own(par, t, fz_s.at[i]).start()
        by_parity(parity, first)
    for copy in mid_copies(c, 0, True, over) + mid_copies(c, 1, True, mate):
        copy.start()

    def pass_on(i):
        def go(par):
            owner = lax.rem(r + 2 * i, R)
            remote(fw.at[f_rows(owner, par)], fw.at[f_rows(owner, par)],
                   fz_s.at[i], fm_r.at[owner], r, c).wait_recv()
            f_pass(owner, par, twin).start()
            f_mate(owner, par).start()
        by_parity(parity, go)

    hidden = silu(split_dot(features[...], time_w[...]))
    tk = time_s.shape[0]
    for q in range(Q):
        @pl.when(c == q)
        def _():
            part[...] = hidden[:, q * tk : (q + 1) * tk]
    emb_own = split_dot(part[...], time_s[...])
    emb[c] = emb_own

    def emb_copy(i, src_c, tgt):
        return remote(emb.at[src_c], emb.at[src_c], emb_s.at[i], emb_r.at[i], r, tgt)

    for i in range(1, Q):
        emb_copy(i, c, lax.rem(c + i, Q)).start()

    for k, (i, j) in enumerate(SIDES):
        @pl.when(inside(r - i, c - j))
        def _():
            lat_copy(k, r - i, c - j).wait_recv()
    where = {side: k for k, side in enumerate(SIDES)}
    for a in range(3):
        tiles = []
        for b in range(3):
            side = (1 - a, 1 - b)
            block = latent[...] if side == (0, 0) else lat[where[side]]
            tiles.append(block.astype(F32))
        wide = jnp.concatenate(tiles, axis=1)
        for b in range(3):
            start = px + b - 1
            patch[cin * (3 * a + b) : cin * (3 * a + b + 1), :] = wide[:, start : start + px]
    skip_feat = dot(patch[...].T.astype(BF16), in_w[...]).astype(BF16)
    deep_t = deep[...].astype(F32).T.astype(BF16)
    own = pl.ds(TILE, px)
    jext[1, own, :] = jnp.concatenate([deep_t.astype(F32), skip_feat.astype(F32)], axis=1).astype(BF16)

    def halo_copy(stage, ext, k, rr, cc):
        i, j = SIDES[k]
        src = ((TILE, TILE), (TILE, px), (px, TILE))[j + 1]
        dst = ((TILE + px, TILE), (TILE, px), (0, TILE))[j + 1]
        return remote(ext.at[1, pl.ds(*src), :], ext.at[1 - i, pl.ds(*dst), :],
                      halo_s.at[stage, k], halo_r.at[stage, k], rr, cc)

    def halo_send(stage, ext):
        for k, (i, j) in enumerate(SIDES):
            @pl.when(inside(r + i, c + j))
            def _():
                halo_copy(stage, ext, k, r + i, c + j).start()

            @pl.when(jnp.logical_not(inside(r - i, c - j)))
            def _():
                dst = ((TILE + px, TILE), (TILE, px), (0, TILE))[j + 1]
                ext[1 - i, pl.ds(*dst), :] = jnp.zeros((dst[1], ext.shape[2]), ext.dtype)

    def halo_wait(stage, ext):
        for k, (i, j) in enumerate(SIDES):
            @pl.when(inside(r - i, c - j))
            def _():
                halo_copy(stage, ext, k, r - i, c - j).wait_recv()

    def indicator(channels, flip):
        shape = (LANES, channels) if flip else (channels, LANES)
        size = channels // GROUPS
        ch = lax.broadcasted_iota(jnp.int32, shape, 1 if flip else 0)
        g = lax.broadcasted_iota(jnp.int32, shape, 0 if flip else 1)
        return ((ch >= g * size) & (ch < g * size + size)).astype(F32)

    def sum_copy(buf, ssem, rsem, stage, slot, i, rr, cc):
        return remote(buf.at[stage, slot], buf.at[stage, slot],
                      ssem.at[stage, i], rsem.at[stage, i], rr, cc)

    def reduce_start(stage, values):
        top = jnp.sum(values, axis=0, keepdims=True)
        low = jnp.sum(values * values, axis=0, keepdims=True)
        both = jnp.concatenate([top, low, jnp.zeros((6, values.shape[1]), F32)], axis=0)
        sums_a[stage, c] = dot(both, indicator(values.shape[1], False), lax.Precision.HIGHEST)
        for i in range(1, Q):
            sum_copy(sums_a, ca_s, ca_r, stage, c, i, r, lax.rem(c + i, Q)).start()

    def reduce_end(stage, channels):
        for i in range(1, Q):
            s = lax.rem(c + Q - i, Q)
            sum_copy(sums_a, ca_s, ca_r, stage, s, i, r, s).wait_recv()
        sums_b[stage, r] = jnp.sum(sums_a[stage], axis=0)
        each(R, lambda i: sum_copy(sums_b, cb_s, cb_r, stage, r, i, lax.rem(r + i, R), c).start())

        def got(i):
            s = lax.rem(r + R - i, R)
            sum_copy(sums_b, cb_s, cb_r, stage, s, i, s, c).wait_recv()

        each(R, got)
        total = jnp.sum(sums_b[stage], axis=0) / (channels // GROUPS * image)
        center = total[0:1]
        inverse = lax.rsqrt(total[1:2] - center * center + EPS)
        both = jnp.concatenate([center, inverse, jnp.zeros((6, LANES), F32)], axis=0)
        wide = dot(both, indicator(channels, True), lax.Precision.HIGHEST)
        return wide[0:1], wide[1:2]

    def conv(stage, ext, stats, gain, weight):
        center, inverse = stats
        channels = ext.shape[2]
        scale = inverse * gain[...]
        place = lax.broadcasted_iota(jnp.int32, (px + 2 * TILE, 1), 0)
        inner = (place >= TILE) & (place < TILE + px)
        total = None
        for a in (1, 0, 2):
            z = (ext[a].astype(F32) - center) * scale
            here = r + a - 1
            keep = (here >= 0) & (here < R) & (
                inner | ((place < TILE) & (c > 0)) | ((place >= TILE + px) & (c < Q - 1)))
            shifted[:, 0:channels] = jnp.where(keep, silu(z), 0.0)
            for b in range(3):
                act = shifted[TILE + b - 1 : TILE + b - 1 + px, 0:channels].astype(BF16)
                k = (3 * a + b) * channels
                term = dot(act, weight[k : k + channels, :])
                total = term if total is None else total + term
        return total

    joined = jext[1, own, :]
    reduce_start(0, joined.astype(F32))
    halo_send(0, jext)

    if ring:
        order = list(range(1, R // 2))
        for i in order[:1]:
            pass_on(i)
    stats = reduce_end(0, 2 * C)
    if ring:
        for i in order[1:]:
            pass_on(i)

        def from_twin(i):
            def go(par):
                owner = lax.rem(twin + 2 * i, R)
                f_pass(owner, par, twin).wait_recv()
                f_mate(owner, par).start()
            by_parity(parity, go)

        for i in range(R // 2):
            from_twin(i)

    for copy in mid_copies(over, 0, False, over):
        copy.wait_recv()
    for copy in mid_copies(over, 2, False, mate):
        copy.start()

    for i in range(1, Q):
        s = lax.rem(c + Q - i, Q)
        emb_copy(i, s, s).wait_recv()
    embedded = jnp.sum(emb[...], axis=0)
    time_shift = split_dot(silu(embedded), time_p[...])

    for copy in locals_:
        copy.wait()
    halo_wait(0, jext)
    if ring:
        def from_mate(i):
            owner = lax.rem(r + i, R)
            def go(par):
                f_mate(owner, 1 - par).wait_recv()
            by_parity(parity, go)
        for i in range(1, R):
            from_mate(i)
    hidden_one = conv(0, jext, stats, gain_one, fw if ring else front) + time_shift

    hext[1, own, :] = hidden_one.astype(BF16)
    reduce_start(1, hidden_one)
    halo_send(1, hext)
    for copy in mid_copies(mate, 1, False, mate):
        copy.wait_recv()
    far = lax.rem(mate + 2, Q)
    for copy in mid_copies(far, 2, False, mate):
        copy.wait_recv()
    shortcut = dot(joined, sw[...])
    stats = reduce_end(1, C)
    halo_wait(1, hext)
    block_out = conv(1, hext, stats, gain_two, mw) + shortcut

    oext[1, own, :] = block_out.astype(BF16)
    reduce_start(2, block_out)
    halo_send(2, oext)
    stats = reduce_end(2, C)
    halo_wait(2, oext)
    result = conv(2, oext, stats, gain_three, out_w)
    noise[...] = result.T[0 : noise.shape[0], :]

    for k, (i, j) in enumerate(SIDES):
        @pl.when(inside(r + i, c + j))
        def _():
            lat_copy(k, r + i, c + j).wait_send()
            for stage, ext in enumerate((jext, hext, oext)):
                halo_copy(stage, ext, k, r + i, c + j).wait_send()
    for i in range(1, Q):
        emb_copy(i, c, lax.rem(c + i, Q)).wait_send()
        for stage in range(3):
            sum_copy(sums_a, ca_s, ca_r, stage, c, i, r, lax.rem(c + i, Q)).wait_send()

    def sent(i):
        for stage in range(3):
            sum_copy(sums_b, cb_s, cb_r, stage, r, i, lax.rem(r + i, R), c).wait_send()

    each(R, sent)
    for copy in (mid_copies(c, 0, True, over) + mid_copies(c, 1, True, mate)
                 + mid_copies(over, 2, False, mate)):
        copy.wait_send()
    if ring:
        def last(par):
            f_own(par, twin, fy_s.at[r]).wait_send()
            for i in range(1, R // 2):
                f_own(par, lax.rem(r + 2 * i, R), fz_s.at[i]).wait_send()
                f_pass(lax.rem(r + 2 * i, R), par, twin).wait_send()
            for i in range(1, R):
                f_mate(lax.rem(r + i, R), par).wait_send()
        by_parity(parity, last)


def shards(
    R, Q,
    latent, deep, timestep, in_weight, front_weight, middle_weight, skip_weight, out_weight,
    time_weight, time_second, time_proj, input_gain, middle_gain, output_gain,
):
    C = deep.shape[0]
    cin = latent.shape[0]
    px = deep.shape[1] * deep.shape[2]
    assert deep.shape[1] == 1 and Q == 4 and R % 2 == 0 and R > 2
    ring = R <= 8 and front_weight.shape[0] % TILE == 0
    half = time_weight.shape[0] // 2
    ratios = jnp.exp(-math.log(10000.0) * jnp.arange(half, dtype=F32) / half)
    angles = timestep[0].astype(F32) * ratios
    features = jnp.concatenate([jnp.cos(angles), jnp.sin(angles)])[None, :]
    front = front_weight if ring else lax.all_gather(front_weight, "rows", axis=0, tiled=True)
    couts = out_weight.shape[1]
    out_w = jnp.pad(out_weight, ((0, 0), (0, LANES - couts)))
    vmem = pl.BlockSpec(memory_space=pltpu.VMEM)
    dma = pltpu.SemaphoreType.DMA
    wide = time_second.shape[1]
    tall = px + 2 * TILE
    args = (
        latent.reshape(cin, px), deep.reshape(C, px), features, in_weight, front,
        middle_weight, skip_weight, out_w, time_weight, time_second, time_proj,
        input_gain[None, :], middle_gain[None, :], output_gain[None, :],
    )
    out = pl.pallas_call(
        functools.partial(kernel, R, Q, ring),
        out_shape=jax.ShapeDtypeStruct((couts, px), F32),
        in_specs=[vmem] * len(args),
        out_specs=vmem,
        scratch_shapes=[
            pltpu.VMEM((8, cin, px), BF16),
            pltpu.VMEM((3, tall, 2 * C), BF16),
            pltpu.VMEM((3, tall, C), BF16),
            pltpu.VMEM((3, tall, C), BF16),
            pltpu.VMEM((tall, 2 * C), F32),
            pltpu.VMEM((9 * cin, px), F32),
            pltpu.VMEM((18 * C if ring else TILE, C), BF16),
            pltpu.VMEM((9 * C, C), BF16),
            pltpu.VMEM((2 * C, C), BF16),
            pltpu.VMEM((1, time_second.shape[0]), F32),
            pltpu.VMEM((Q, 1, wide), F32),
            pltpu.VMEM((3, Q, 8, LANES), F32),
            pltpu.VMEM((3, R, 8, LANES), F32),
            dma((8,)), dma((8,)), dma((3, 8)), dma((3, 8)),
            dma((R,)), dma((R,)), dma((R,)), dma((R,)), dma((R,)),
            dma((2, 3)), dma((2, 3)), dma((Q,)), dma((Q,)),
            dma((3, Q)), dma((3, Q)), dma((3, R)), dma((3, R)), dma((3,)),
        ],
        compiler_params=pltpu.CompilerParams(
            collective_id=0, has_side_effects=True, vmem_limit_bytes=56 * 1024 * 1024
        ),
    )(*args)
    return out.reshape(couts, 1, px)


def solution(mesh):
    R, Q = mesh.shape["rows"], mesh.shape["cols"]
    return jax.shard_map(
        functools.partial(shards, R, Q),
        mesh=mesh,
        in_specs=(
            P(None, "rows", "cols"), P(None, "rows", "cols"), P(), P(),
            P("rows", None), P("cols", None), P("cols", None), P(),
            P(), P("cols", None), P(), P(), P(), P(),
        ),
        out_specs=P(None, "rows", "cols"),
        check_vma=False,
    )
```

```python
import functools
import math

import jax
import jax.numpy as jnp
from jax import lax
from jax.experimental import pallas as pl
from jax.experimental.pallas import tpu as pltpu
from jax.sharding import PartitionSpec as P

GROUPS = 32
EPS = 1e-05
TILE = 16
LANES = 128
MESH = pl.DeviceIdType.MESH
F32 = jnp.float32
BF16 = jnp.bfloat16
SIDES = tuple((i, j) for i in (-1, 0, 1) for j in (-1, 0, 1) if (i, j) != (0, 0))


def dot(a, b, precision=None):
    return lax.dot_general(
        a, b, (((1,), (0,)), ((), ())), preferred_element_type=F32, precision=precision
    )


def split_dot(row, weight):
    high = row.astype(BF16)
    rest = row - high.astype(F32)
    middle = rest.astype(BF16)
    low = (rest - middle.astype(F32)).astype(BF16)
    pieces = jnp.concatenate([high.astype(F32), middle.astype(F32), low.astype(F32)], axis=0)
    return jnp.sum(dot(pieces.astype(BF16), weight), axis=0, keepdims=True)


def silu(z):
    return z / (1.0 + jnp.exp(-z))


def kernel(
    R, Q, ring,
    latent, deep, rows_in, in_w, front, middle, skip, out_w, time_w, time_s, time_p,
    noise,
    lat, jext, hext, oext, shifted, patch, fw, mw, sw, part, emb, sums_a, sums_b,
    lat_s, lat_r, halo_s, halo_r, fz_s, fy_s, fc_s, fm_r, fo_r, mid_s, mid_r, emb_s, emb_r,
    ca_s, ca_r, cb_s, cb_r, loc_s,
):
    r = lax.axis_index("rows")
    c = lax.axis_index("cols")
    C, px = deep.shape
    cin = latent.shape[0]
    image = float(px * R * Q)
    FQ = time_w.shape[0]
    gain_one = rows_in[:, FQ : FQ + 2 * C]
    gain_two = rows_in[:, FQ + 2 * C : FQ + 3 * C]
    gain_three = rows_in[:, FQ + 3 * C : FQ + 4 * C]

    def remote(src, dst, ssem, rsem, rr, cc):
        return pltpu.make_async_remote_copy(
            src_ref=src, dst_ref=dst, send_sem=ssem, recv_sem=rsem,
            device_id={"rows": rr, "cols": cc}, device_id_type=MESH,
        )

    def each(count, body):
        if count <= 8:
            for i in range(1, count):
                body(i)
        else:
            lax.fori_loop(1, count, lambda i, u: (body(i), u)[1], 0)

    barrier = pltpu.get_barrier_semaphore()

    def greet(rr, cc):
        pl.semaphore_signal(barrier, inc=1, device_id={"rows": rr, "cols": cc}, device_id_type=MESH)

    each(R, lambda i: greet(lax.rem(r + i, R), c))
    each(Q, lambda i: greet(r, lax.rem(c + i, Q)))
    for i in (-1, 1):
        for j in (-1, 1):
            greet(lax.rem(r + i + R, R), lax.rem(c + j + Q, Q))
    pl.semaphore_wait(barrier, R - 1 + Q - 1 + 4)

    def inside(rr, cc):
        return (rr >= 0) & (rr < R) & (cc >= 0) & (cc < Q)

    def lat_copy(k, rr, cc):
        i, j = SIDES[k]
        return remote(latent, lat.at[k], lat_s.at[k], lat_r.at[k], rr, cc)

    for k, (i, j) in enumerate(SIDES):
        @pl.when(inside(r + i, c + j))
        def _():
            lat_copy(k, r + i, c + j).start()

        @pl.when(jnp.logical_not(inside(r - i, c - j)))
        def _():
            lat[k] = jnp.zeros(lat.shape[1:], lat.dtype)

    parity = lax.rem(c, 2)
    mate = c + 1 - 2 * parity
    over = lax.rem(c + 2, Q)
    half_c = lax.rem(r, 2)
    twin = r + 1 - 2 * half_c
    mk, sk = middle.shape[0], skip.shape[0]

    def mid_copies(owner, s, slot_from, target):
        rows_m = pl.ds(pl.multiple_of(owner * mk, TILE), mk)
        rows_s = pl.ds(pl.multiple_of(owner * sk, TILE), sk)
        src_m, src_s = (middle, skip) if slot_from else (mw.at[rows_m], sw.at[rows_s])
        return (
            remote(src_m, mw.at[rows_m], mid_s.at[0, s], mid_r.at[0, s], r, target),
            remote(src_s, sw.at[rows_s], mid_s.at[1, s], mid_r.at[1, s], r, target),
        )

    fk = fw.shape[0] // R if ring else 0
    cut = fk // 2 // TILE * TILE
    spans = ((0, cut), (cut, fk - cut))

    def f_rows(owner, par):
        return pl.ds(pl.multiple_of(owner * fk, TILE) + spans[par][0], spans[par][1])

    def by_parity(par_of, body):
        for par in (0, 1):
            @pl.when(par_of == par)
            def _():
                body(par)

    def f_own(par, target, ssem):
        src = front.at[pl.ds(spans[par][0], spans[par][1])]
        return remote(src, fw.at[f_rows(r, par)], ssem, fm_r.at[r], target, c)

    def f_pass(owner, par, target):
        return remote(fw.at[f_rows(owner, par)], fw.at[f_rows(owner, par)],
                      fy_s.at[owner], fm_r.at[owner], target, c)

    def f_mate(owner, par):
        return remote(fw.at[f_rows(owner, par)], fw.at[f_rows(owner, par)],
                      fc_s.at[owner], fo_r.at[owner], r, mate)

    def by_distance(distances, body):
        for d in distances:
            for t in (r + 2 * d, r - 2 * d):
                @pl.when((t >= 0) & (t < R))
                def _():
                    body(t)

    locals_ = []
    if ring:
        locals_.append(pltpu.make_async_copy(
            front, fw.at[pl.ds(pl.multiple_of(r * fk, TILE), fk)], loc_s.at[0]))
    locals_.append(pltpu.make_async_copy(
        middle, mw.at[pl.ds(pl.multiple_of(c * mk, TILE), mk)], loc_s.at[1]))
    locals_.append(pltpu.make_async_copy(
        skip, sw.at[pl.ds(pl.multiple_of(c * sk, TILE), sk)], loc_s.at[2]))
    for copy in locals_:
        copy.start()

    if ring:
        def first(par):
            f_own(par, twin, fy_s.at[r]).start()
            def one(t):
                f_own(par, t, fz_s.at[t]).start()
            by_distance(range(1, R // 2), one)
        by_parity(parity, first)
    for copy in mid_copies(c, 0, True, over) + mid_copies(c, 1, True, mate):
        copy.start()

    def pass_on(distances):
        def go(par):
            def one(owner):
                f_pass(owner, par, twin).wait_recv()
                f_pass(owner, par, twin).start()
                f_mate(owner, par).start()
            by_distance(distances, one)
        by_parity(parity, go)

    for k, (i, j) in enumerate(SIDES):
        @pl.when(inside(r - i, c - j))
        def _():
            lat_copy(k, r - i, c - j).wait_recv()
    where = {side: k for k, side in enumerate(SIDES)}
    for a in range(3):
        tiles = []
        for b in range(3):
            side = (1 - a, 1 - b)
            block = latent[...] if side == (0, 0) else lat[where[side]]
            tiles.append(block.astype(F32))
        wide = jnp.concatenate(tiles, axis=1)
        for b in range(3):
            start = px + b - 1
            patch[cin * (3 * a + b) : cin * (3 * a + b + 1), :] = wide[:, start : start + px]
    skip_feat = dot(patch[...].T.astype(BF16), in_w[...]).astype(BF16)
    deep_t = deep[...].astype(F32).T.astype(BF16)
    own = pl.ds(TILE, px)
    jext[1, own, :] = jnp.concatenate([deep_t.astype(F32), skip_feat.astype(F32)], axis=1).astype(BF16)

    def halo_copy(stage, ext, k, rr, cc):
        i, j = SIDES[k]
        src = ((TILE, TILE), (TILE, px), (px, TILE))[j + 1]
        dst = ((TILE + px, TILE), (TILE, px), (0, TILE))[j + 1]
        return remote(ext.at[1, pl.ds(*src), :], ext.at[1 - i, pl.ds(*dst), :],
                      halo_s.at[stage, k], halo_r.at[stage, k], rr, cc)

    def halo_send(stage, ext):
        for k, (i, j) in enumerate(SIDES):
            @pl.when(inside(r + i, c + j))
            def _():
                halo_copy(stage, ext, k, r + i, c + j).start()

            @pl.when(jnp.logical_not(inside(r - i, c - j)))
            def _():
                dst = ((TILE + px, TILE), (TILE, px), (0, TILE))[j + 1]
                ext[1 - i, pl.ds(*dst), :] = jnp.zeros((dst[1], ext.shape[2]), ext.dtype)

    def halo_wait(stage, ext):
        for k, (i, j) in enumerate(SIDES):
            @pl.when(inside(r - i, c - j))
            def _():
                halo_copy(stage, ext, k, r - i, c - j).wait_recv()

    def indicator(channels, flip):
        shape = (LANES, channels) if flip else (channels, LANES)
        size = channels // GROUPS
        ch = lax.broadcasted_iota(jnp.int32, shape, 1 if flip else 0)
        g = lax.broadcasted_iota(jnp.int32, shape, 0 if flip else 1)
        return ((ch >= g * size) & (ch < g * size + size)).astype(F32)

    def sum_copy(buf, ssem, rsem, stage, slot, i, rr, cc):
        return remote(buf.at[stage, slot], buf.at[stage, slot],
                      ssem.at[stage, i], rsem.at[stage, i], rr, cc)

    def reduce_start(stage, values):
        top = jnp.sum(values, axis=0, keepdims=True)
        low = jnp.sum(values * values, axis=0, keepdims=True)
        both = jnp.concatenate([top, low, jnp.zeros((6, values.shape[1]), F32)], axis=0)
        sums_a[stage, c] = dot(both, indicator(values.shape[1], False), lax.Precision.HIGHEST)
        for i in range(1, Q):
            sum_copy(sums_a, ca_s, ca_r, stage, c, i, r, lax.rem(c + i, Q)).start()

    def reduce_end(stage, channels):
        for i in range(1, Q):
            s = lax.rem(c + Q - i, Q)
            sum_copy(sums_a, ca_s, ca_r, stage, s, i, r, s).wait_recv()
        sums_b[stage, r] = jnp.sum(sums_a[stage], axis=0)
        each(R, lambda i: sum_copy(sums_b, cb_s, cb_r, stage, r, i, lax.rem(r + i, R), c).start())

        def got(i):
            s = lax.rem(r + R - i, R)
            sum_copy(sums_b, cb_s, cb_r, stage, s, i, s, c).wait_recv()

        each(R, got)
        total = jnp.sum(sums_b[stage], axis=0) / (channels // GROUPS * image)
        center = total[0:1]
        inverse = lax.rsqrt(total[1:2] - center * center + EPS)
        both = jnp.concatenate([center, inverse, jnp.zeros((6, LANES), F32)], axis=0)
        wide = dot(both, indicator(channels, True), lax.Precision.HIGHEST)
        return wide[0:1], wide[1:2]

    def conv(ext, stats, gain, weight, exact=None, shift=None):
        center, inverse = stats
        if shift is not None:
            center = center - shift
        channels = ext.shape[2]
        scale = inverse * gain
        place = lax.broadcasted_iota(jnp.int32, (px + 2 * TILE, 1), 0)
        inner = (place >= TILE) & (place < TILE + px)
        total = None
        for a in (1, 0, 2):
            z = (ext[a].astype(F32) - center) * scale
            here = r + a - 1
            keep = (here >= 0) & (here < R) & (
                inner | ((place < TILE) & (c > 0)) | ((place >= TILE + px) & (c < Q - 1)))
            shifted[:, 0:channels] = jnp.where(keep, silu(z), 0.0)
            if a == 1 and exact is not None:
                shifted[own, 0:channels] = silu((exact - center) * scale)
            for b in range(3):
                act = shifted[TILE + b - 1 : TILE + b - 1 + px, 0:channels].astype(BF16)
                k = (3 * a + b) * channels
                term = dot(act, weight[k : k + channels, :])
                total = term if total is None else total + term
        return total

    joined = jext[1, own, :]
    reduce_start(0, joined.astype(F32))
    halo_send(0, jext)

    hidden = silu(split_dot(rows_in[:, 0:FQ], time_w[...]))
    tk = time_s.shape[0]
    for q in range(Q):
        @pl.when(c == q)
        def _():
            part[...] = hidden[:, q * tk : (q + 1) * tk]
    emb_own = split_dot(part[...], time_s[...])
    emb[c] = emb_own

    def emb_copy(i, src_c, tgt):
        return remote(emb.at[src_c], emb.at[src_c], emb_s.at[i], emb_r.at[i], r, tgt)

    for i in range(1, Q):
        emb_copy(i, c, lax.rem(c + i, Q)).start()

    if ring:
        pass_on((1,))
    stats = reduce_end(0, 2 * C)
    if ring:
        pass_on(range(2, R // 2))

        def from_twin(par):
            def one(t):
                owner = t + twin - r
                f_pass(owner, par, twin).wait_recv()
                f_mate(owner, par).start()
            one(r)
            by_distance(range(1, R // 2), one)
        by_parity(parity, from_twin)

    for copy in mid_copies(over, 0, False, over):
        copy.wait_recv()
    for copy in mid_copies(over, 2, False, mate):
        copy.start()

    for i in range(1, Q):
        s = lax.rem(c + Q - i, Q)
        emb_copy(i, s, s).wait_recv()
    embedded = jnp.sum(emb[...], axis=0)
    time_shift = split_dot(silu(embedded), time_p[...])

    for copy in locals_:
        copy.wait()
    halo_wait(0, jext)
    if ring:
        def from_mate(i):
            owner = lax.rem(r + i, R)
            def go(par):
                f_mate(owner, 1 - par).wait_recv()
            by_parity(parity, go)
        for i in range(1, R):
            from_mate(i)
    front_out = conv(jext, stats, gain_one, fw if ring else front)

    hext[1, own, :] = front_out.astype(BF16)
    reduce_start(1, front_out + time_shift)
    halo_send(1, hext)
    for copy in mid_copies(mate, 1, False, mate):
        copy.wait_recv()
    far = lax.rem(mate + 2, Q)
    for copy in mid_copies(far, 2, False, mate):
        copy.wait_recv()
    shortcut = dot(joined, sw[...])
    stats = reduce_end(1, C)
    halo_wait(1, hext)
    block_out = conv(hext, stats, gain_two, mw, front_out, time_shift) + shortcut

    oext[1, own, :] = block_out.astype(BF16)
    reduce_start(2, block_out)
    halo_send(2, oext)
    stats = reduce_end(2, C)
    halo_wait(2, oext)
    result = conv(oext, stats, gain_three, out_w, block_out)
    noise[...] = result.T[0 : noise.shape[0], :]

    for k, (i, j) in enumerate(SIDES):
        @pl.when(inside(r + i, c + j))
        def _():
            lat_copy(k, r + i, c + j).wait_send()
            for stage, ext in enumerate((jext, hext, oext)):
                halo_copy(stage, ext, k, r + i, c + j).wait_send()
    for i in range(1, Q):
        emb_copy(i, c, lax.rem(c + i, Q)).wait_send()
        for stage in range(3):
            sum_copy(sums_a, ca_s, ca_r, stage, c, i, r, lax.rem(c + i, Q)).wait_send()

    def sent(i):
        for stage in range(3):
            sum_copy(sums_b, cb_s, cb_r, stage, r, i, lax.rem(r + i, R), c).wait_send()

    each(R, sent)
    for copy in (mid_copies(c, 0, True, over) + mid_copies(c, 1, True, mate)
                 + mid_copies(over, 2, False, mate)):
        copy.wait_send()
    if ring:
        def last(par):
            f_own(par, twin, fy_s.at[r]).wait_send()
            def one(t):
                f_own(par, t, fz_s.at[t]).wait_send()
                f_pass(t, par, twin).wait_send()
            by_distance(range(1, R // 2), one)
            for i in range(1, R):
                f_mate(lax.rem(r + i, R), par).wait_send()
        by_parity(parity, last)


def shards(
    R, Q,
    latent, deep, timestep, in_weight, front_weight, middle_weight, skip_weight, out_weight,
    time_weight, time_second, time_proj, input_gain, middle_gain, output_gain,
):
    C = deep.shape[0]
    cin = latent.shape[0]
    px = deep.shape[1] * deep.shape[2]
    assert deep.shape[1] == 1 and Q == 4 and R % 2 == 0 and R > 2
    ring = R <= 8 and front_weight.shape[0] % TILE == 0
    half = time_weight.shape[0] // 2
    ratios = jnp.exp(-math.log(10000.0) * jnp.arange(half, dtype=F32) / half)
    angles = timestep[0].astype(F32) * ratios
    rows_in = jnp.concatenate(
        [jnp.cos(angles), jnp.sin(angles), input_gain, middle_gain, output_gain])[None, :]
    front = front_weight if ring else lax.all_gather(front_weight, "rows", axis=0, tiled=True)
    couts = out_weight.shape[1]
    out_w = jnp.pad(out_weight, ((0, 0), (0, LANES - couts)))
    vmem = pl.BlockSpec(memory_space=pltpu.VMEM)
    dma = pltpu.SemaphoreType.DMA
    wide = time_second.shape[1]
    tall = px + 2 * TILE
    args = (
        latent.reshape(cin, px), deep.reshape(C, px), rows_in, in_weight, front,
        middle_weight, skip_weight, out_w, time_weight, time_second, time_proj,
    )
    out = pl.pallas_call(
        functools.partial(kernel, R, Q, ring),
        out_shape=jax.ShapeDtypeStruct((couts, px), F32),
        in_specs=[vmem] * len(args),
        out_specs=vmem,
        scratch_shapes=[
            pltpu.VMEM((8, cin, px), BF16),
            pltpu.VMEM((3, tall, 2 * C), BF16),
            pltpu.VMEM((3, tall, C), BF16),
            pltpu.VMEM((3, tall, C), BF16),
            pltpu.VMEM((tall, 2 * C), F32),
            pltpu.VMEM((9 * cin, px), F32),
            pltpu.VMEM((18 * C if ring else TILE, C), BF16),
            pltpu.VMEM((9 * C, C), BF16),
            pltpu.VMEM((2 * C, C), BF16),
            pltpu.VMEM((1, time_second.shape[0]), F32),
            pltpu.VMEM((Q, 1, wide), F32),
            pltpu.VMEM((3, Q, 8, LANES), F32),
            pltpu.VMEM((3, R, 8, LANES), F32),
            dma((8,)), dma((8,)), dma((3, 8)), dma((3, 8)),
            dma((R,)), dma((R,)), dma((R,)), dma((R,)), dma((R,)),
            dma((2, 3)), dma((2, 3)), dma((Q,)), dma((Q,)),
            dma((3, Q)), dma((3, Q)), dma((3, R)), dma((3, R)), dma((3,)),
        ],
        compiler_params=pltpu.CompilerParams(
            collective_id=0, has_side_effects=True, vmem_limit_bytes=56 * 1024 * 1024
        ),
    )(*args)
    return out.reshape(couts, 1, px)


def solution(mesh):
    R, Q = mesh.shape["rows"], mesh.shape["cols"]
    return jax.shard_map(
        functools.partial(shards, R, Q),
        mesh=mesh,
        in_specs=(
            P(None, "rows", "cols"), P(None, "rows", "cols"), P(), P(),
            P("rows", None), P("cols", None), P("cols", None), P(),
            P(), P("cols", None), P(), P(), P(), P(),
        ),
        out_specs=P(None, "rows", "cols"),
        check_vma=False,
    )
```
